32 devices in a mesh: gx: 4 (over x, core), gy: 4 (over z), gz: 2 (over y).
Axes of the slice: x: 2, y: 2, z: 4, core: 2. Of those that a mesh axis runs over, the one named last changes fastest.
Arguments:
- particle_fields: float32 [20, 262144], P(None, ('gx', 'gy', 'gz')), may hold values from -4 to 4
- step_length: float32 [262144], P(('gx', 'gy', 'gz')), may hold values from 0.1 to 1
- live_mask: int32 [262144], P(('gx', 'gy', 'gz')), may hold values 0 or 1
- dest_cell: int32 [262144], P(('gx', 'gy', 'gz')), may hold values from 0 to 511
- block_counts: int32 [32, 6], P(('gx', 'gy', 'gz')), may hold values from 0 to 12, as said below
- block_lists: int32 [32, 48], P(('gx', 'gy', 'gz')), may hold values from 0 to 87, as said below
Outputs:
- tile_sums: float32 [20, 16384], P(None, ('gx', 'gy', 'gz'))
The draws below stay inside these ranges and needn't reach their ends.
Inputs may be any that keep to these rules, and one draw needn't show every extreme that they name: `block_counts`: columns are directions in the order x lower, x upper, z lower, z upper, y lower, y upper; a count is at most its section's span (6, 6 or 12) and may be 0; at every section some domain receives full spans from both neighbours. `block_lists`: per domain, 6 entries toward the lower x neighbour, 6 toward the upper, then 2 * 6 for z and 24 for y in the same way; entries are block numbers of the domain's pool at that section. Entries below their direction's count are valid: valid entries of one domain over all sections are distinct, and each names an own block or an appended block that its sender filled. Other entries are arbitrary numbers within the pool.
All inputs are finite; a program needn't handle non-finite values. No bound on the sum of `live_mask` on one device may be relied on, other than what follows from the above.
Results may differ from the reference program's by a relative error of at most 0.0003.
Values sent between devices are 32-bit elements; how exact they have to be, the bound alone decides.
A program may use at most 64 MiB of HBM per device.

```python
import math
import jax
import jax.numpy as jnp

FIELDS = 20
BLOCKS = 64
CELLS = 512
CAP_X = 6
CAP_Z = 6
CAP_Y = 12
LIST_LEN = 48
PARTICLES = 262144
N_GX = 4
N_GY = 4
N_GZ = 2


def plan_migration(key):
    shape_grid = (N_GX, N_GY, N_GZ)
    final_count = BLOCKS + 2 * (CAP_X + CAP_Z + CAP_Y)
    pool_index = jnp.arange(final_count, dtype=jnp.int32)
    eligible = jnp.broadcast_to(pool_index < BLOCKS, shape_grid + (final_count,))
    coords = jnp.meshgrid(jnp.arange(N_GX, dtype=jnp.int32), jnp.arange(N_GY, dtype=jnp.int32), jnp.arange(N_GZ, dtype=jnp.int32), indexing='ij')
    extents_grid = jnp.array(shape_grid, dtype=jnp.int32)
    size_now = BLOCKS
    count_parts = []
    list_parts = []
    for section_index, (axis_place, extent) in enumerate(((0, CAP_X), (2, CAP_Z), (1, CAP_Y))):
        section_key = jax.random.fold_in(key, 101 + section_index)
        count_key, pick_key, filler_key, target_key = jax.random.split(section_key, 4)
        rough_draw = jax.random.randint(count_key, shape_grid + (2,), 0, extent + 1, dtype=jnp.int32)
        number = rough_draw * rough_draw // extent
        target = jax.random.randint(target_key, (3,), 0, extents_grid, dtype=jnp.int32)
        step_unit = (jnp.arange(3) == axis_place).astype(jnp.int32)
        lower_site = (target - step_unit) % extents_grid
        upper_site = (target + step_unit) % extents_grid
        at_lower = (coords[0] == lower_site[0]) & (coords[1] == lower_site[1]) & (coords[2] == lower_site[2])
        at_upper = (coords[0] == upper_site[0]) & (coords[1] == upper_site[1]) & (coords[2] == upper_site[2])
        toward_lower = jnp.where(at_upper, extent, number[..., 0]).astype(jnp.int32)
        toward_upper = jnp.where(at_lower, extent, number[..., 1]).astype(jnp.int32)
        scores = jax.random.randint(pick_key, shape_grid + (final_count,), 0, 1 << 20, dtype=jnp.int32) * final_count + pool_index
        scores = jnp.where(eligible, scores, -1)
        chosen = jnp.argsort(-scores, axis=-1)[..., :2 * extent].astype(jnp.int32)
        position = jnp.arange(2 * extent) % extent
        wanted = jnp.where(jnp.arange(2 * extent) < extent, toward_lower[..., None], toward_upper[..., None])
        usable = position < wanted
        filler = jax.random.randint(filler_key, shape_grid + (2 * extent,), 0, size_now, dtype=jnp.int32)
        list_parts.append(jnp.where(usable, chosen, filler))
        count_parts.append(jnp.stack([toward_lower, toward_upper], axis=-1))
        taken_now = jnp.any((chosen[..., :, None] == pool_index) & usable[..., None], axis=-2)
        from_lower = jnp.roll(toward_upper, 1, axis=axis_place)
        from_upper = jnp.roll(toward_lower, -1, axis=axis_place)
        offset = pool_index - size_now
        landed = (offset >= 0) & (offset < extent) & (offset < from_lower[..., None]) | (offset >= extent) & (offset < 2 * extent) & (offset - extent < from_upper[..., None])
        eligible = eligible & jnp.logical_not(taken_now) | landed
        size_now = size_now + 2 * extent
    counts = jnp.concatenate(count_parts, axis=-1).reshape(N_GX * N_GY * N_GZ, 6)
    entries = jnp.concatenate(list_parts, axis=-1).reshape(N_GX * N_GY * N_GZ, 2 * (CAP_X + CAP_Z + CAP_Y))
    return (counts.astype(jnp.int32), entries.astype(jnp.int32))


def draw_block_counts(key, part):
    return plan_migration(key)[0]


def draw_block_lists(key, part):
    return plan_migration(key)[1]


def set_ends(values, stream_key, low, high):
    dims = values.shape
    place = [jax.random.randint(jax.random.fold_in(stream_key, axis), (), 0, dims[axis]) for axis in range(len(dims))]
    values = values.at[tuple(place)].set(low)
    longest = dims.index(max(dims))
    place[longest] = (place[longest] + 1) % dims[longest]
    return values.at[tuple(place)].set(high)


def levels(stream_key, dims, pieces, least, high):
    loudness, own = 1.0, jax.random.fold_in(stream_key, 6)
    for axis_at, shards_of in pieces:
        steps = jnp.exp(jax.random.uniform(jax.random.fold_in(own, axis_at), (shards_of,), jnp.float32, least / len(pieces), high / len(pieces)))
        loudness = loudness * jnp.repeat(steps, dims[axis_at] // shards_of).reshape([-1 if axis == axis_at else 1 for axis in range(len(dims))])
    return loudness


def centred(rng, shape, deviation, reach, cuts=(), kind=jnp.bfloat16):
    values = jax.random.normal(rng, shape, jnp.float32) * deviation
    if len(cuts) > 0:
        values = levels(rng, shape, cuts, -0.22, 0.18) * values
    return jnp.clip(values, min=-reach, max=reach).astype(kind)


def setup_inputs(seed: int = 0) -> dict:
    arg_keys = jax.random.split(jax.random.key(seed), 7)
    return {
        "particle_fields": centred(arg_keys[0], (FIELDS, PARTICLES), 0.25, 4.0, ((1, 32),), jnp.float32),
        "step_length": jnp.clip(jnp.exp(math.log(1.0) - 2.3025851 * jax.random.uniform(arg_keys[1], (PARTICLES,), jnp.float32) ** levels(arg_keys[1], (PARTICLES,), ((0, 32),), -0.2, 0.2)), 0.1, 1.0),
        "live_mask": set_ends((jax.random.randint(arg_keys[2], (PARTICLES,), 0, 4) < 3).astype(jnp.int32), jax.random.fold_in(arg_keys[2], 1), 0, 1),
        "dest_cell": set_ends(jax.random.randint(arg_keys[3], (PARTICLES,), 0, CELLS), jax.random.fold_in(arg_keys[3], 1), 0, CELLS - 1).astype(jnp.int32),
        "block_counts": draw_block_counts(jax.random.fold_in(arg_keys[6], 71), 0),
        "block_lists": draw_block_lists(jax.random.fold_in(arg_keys[6], 71), 0),
    }


def leave_section(holding, chosen, number, axis_place):
    extent = chosen.shape[-1] // 2
    index_full = jnp.broadcast_to(chosen.astype(jnp.int32)[None, :, :, :, :, None], holding.shape[:4] + (2 * extent, 128))
    picked = jnp.take_along_axis(holding, index_full, axis=4)
    position = jnp.arange(2 * extent) % extent
    wanted = jnp.where(jnp.arange(2 * extent) < extent, number[..., 0:1], number[..., 1:2])
    usable = (position < wanted).astype(jnp.float32)
    outgoing = picked * usable[None, :, :, :, :, None]
    from_lower = jnp.roll(outgoing[:, :, :, :, extent:], 1, axis=axis_place + 1)
    from_upper = jnp.roll(outgoing[:, :, :, :, :extent], -1, axis=axis_place + 1)
    return jnp.concatenate([holding, from_lower, from_upper], axis=4)


def reference(particle_fields, step_length, live_mask, dest_cell, block_counts, block_lists):
    advanced = particle_fields[0:3] + step_length[None, :] * particle_fields[3:6]
    carried = jnp.concatenate([advanced, particle_fields[3:], live_mask.astype(jnp.float32)[None, :], dest_cell.astype(jnp.float32)[None, :]], axis=0)
    row_count = FIELDS + 2
    domain_count = N_GX * N_GY * N_GZ
    holding = carried.reshape(row_count, N_GX, N_GY, N_GZ, BLOCKS, 128)
    number = block_counts.reshape(N_GX, N_GY, N_GZ, 6)
    entries = block_lists.reshape(N_GX, N_GY, N_GZ, LIST_LEN)
    first_end = 2 * CAP_X
    second_end = first_end + 2 * CAP_Z
    holding = leave_section(holding, entries[..., :first_end], number[..., 0:2], 0)
    holding = leave_section(holding, entries[..., first_end:second_end], number[..., 2:4], 2)
    before_count = holding.shape[4]
    holding = leave_section(holding, entries[..., second_end:], number[..., 4:6], 1)
    spans = (CAP_X, CAP_X, CAP_Z, CAP_Z, CAP_Y, CAP_Y)
    limits = [jnp.broadcast_to(number[..., column:column + 1], (N_GX, N_GY, N_GZ, extent)) for column, extent in enumerate(spans)]
    wanted = jnp.concatenate(limits, axis=-1)
    position = jnp.concatenate([jnp.arange(extent) for extent in spans])
    listed = (entries[..., :, None] == jnp.arange(before_count)[None, None, None, None, :]) & (position < wanted)[..., None]
    keep_before = 1.0 - jnp.any(listed, axis=3).astype(jnp.float32)
    keep_block = jnp.concatenate([keep_before, jnp.ones((N_GX, N_GY, N_GZ, holding.shape[4] - before_count), jnp.float32)], axis=-1)
    weights = holding[FIELDS] * keep_block[..., None]
    domain = jnp.arange(domain_count, dtype=jnp.int32).reshape(N_GX, N_GY, N_GZ, 1, 1)
    segment = (domain * CELLS + holding[FIELDS + 1].astype(jnp.int32)).reshape(-1)
    columns = []
    for field_index in range(FIELDS):
        columns.append(jax.ops.segment_sum((holding[field_index] * weights).reshape(-1), segment, num_segments=domain_count * CELLS))
    return jnp.stack(columns, axis=0)
```

```python
import functools

import jax
import jax.numpy as jnp
from jax import lax
from jax.experimental import pallas as pl
from jax.experimental.pallas import tpu as pltpu
from jax.sharding import PartitionSpec as P

CELLS = 512
CAP_X = 6
CAP_Z = 6
CAP_Y = 12
LANES = 128
HALF = 256
GROUP = 8
GONE = 8 * CELLS
CLASSES = 3


def migrate_kernel(
    sizes,
    counts,
    lists,
    lists_row,
    fields_hbm,
    step_hbm,
    live_hbm,
    cell_hbm,
    out_ref,
    fields,
    step,
    live,
    cell,
    pool,
    offsets,
    acc,
    sent_x,
    sent_z,
    got_x,
    got_z,
    sent_y,
    got_y,
    load_sem,
    send_sem,
    recv_sem,
):
    field_count = fields_hbm.shape[0]
    rows = sent_x.shape[1]
    blocks = step.shape[0]

    me = {axis: lax.axis_index(axis) for axis in ("gx", "gy", "gz")}
    lower = {axis: {axis: lax.rem(me[axis] + sizes[axis] - 1, sizes[axis])} for axis in me}
    upper = {axis: {axis: lax.rem(me[axis] + 1, sizes[axis])} for axis in me}

    loads = [
        pltpu.make_async_copy(fields_hbm, fields, load_sem.at[0]),
        pltpu.make_async_copy(step_hbm, step, load_sem.at[1]),
        pltpu.make_async_copy(live_hbm, live, load_sem.at[2]),
        pltpu.make_async_copy(cell_hbm, cell, load_sem.at[3]),
    ]
    for load in loads:
        load.start()

    barrier = pltpu.get_barrier_semaphore()
    for axis in me:
        for neighbour in (lower[axis], upper[axis]):
            pl.semaphore_signal(
                barrier, inc=1, device_id=neighbour, device_id_type=pl.DeviceIdType.MESH
            )

    spans = (CAP_X, CAP_X, CAP_Z, CAP_Z, CAP_Y, CAP_Y)
    lane = lax.broadcasted_iota(jnp.int32, lists_row.shape, 1)
    limit = jnp.zeros(lists_row.shape, jnp.int32)
    away = jnp.zeros(lists_row.shape, jnp.float32)
    start = 0
    for k, span in enumerate(spans):
        here = lane >= start
        limit = jnp.where(here, counts[0, k] + start, limit)
        away = jnp.where(here, float(GONE if k < 4 else (k - 3) * CELLS), away)
        start += span
    away = jnp.where(lane < limit, away, 0.0)
    number = lax.broadcasted_iota(jnp.int32, (offsets.shape[0], lists_row.shape[1]), 0)
    named = jnp.where(lists_row[...] == number, away, 0.0)
    offsets[...] = jnp.broadcast_to(jnp.sum(named, axis=1, keepdims=True), offsets.shape)

    for load in loads:
        load.wait()

    first_row = lax.broadcasted_iota(jnp.int32, (8, LANES), 0)

    def own_block(e):
        v = fields[:, pl.ds(pl.multiple_of(e * LANES, LANES), LANES)]
        top = v[:8]
        pace = step[pl.ds(e, 1), :]
        top = top + jnp.where(first_row < 3, pace * pltpu.roll(top, 5, 0), 0.0)
        v = jnp.concatenate([top, v[8:]], axis=0)
        v = v * live[pl.ds(e, 1), :].astype(jnp.float32)
        where_to = cell[pl.ds(e, 1), :].astype(jnp.float32)
        return jnp.concatenate(
            [v, jnp.broadcast_to(where_to, (rows - field_count, LANES))], axis=0
        )

    def exchange(axis, index, sent, got, width):
        out = []
        for side, (target, other) in enumerate(((lower, 1), (upper, 0))):
            copy = pltpu.make_async_remote_copy(
                src_ref=sent.at[pl.ds(side * width, width)],
                dst_ref=got.at[pl.ds(other * width, width)],
                send_sem=send_sem.at[index + side],
                recv_sem=recv_sem.at[index + other],
                device_id=target[axis],
                device_id_type=pl.DeviceIdType.MESH,
            )
            copy.start()
            out.append(copy)
        return out

    def fill(sent, slot, span, first_entry, first_count):
        count = jnp.full((rows, LANES), counts[0, first_count + slot // span])
        block = pool[lists[0, first_entry + slot]]
        sent[slot] = jnp.where(count > slot % span, block, 0.0)

    def advance(g, carry):
        for i in range(GROUP):
            pool[g * GROUP + i] = own_block(g * GROUP + i)
        return carry

    lax.fori_loop(0, blocks // GROUP, advance, 0)
    for slot in range(2 * CAP_X):
        fill(sent_x, slot, CAP_X, 0, 0)
    pl.semaphore_wait(barrier, 6)
    copies_x = exchange("gx", 0, sent_x, got_x, CAP_X)

    code = lax.broadcasted_iota(jnp.int32, (HALF, LANES), 0).astype(jnp.float32)
    parts = CLASSES * CELLS // HALF

    def operands(v, cells):
        high = v.astype(jnp.bfloat16).astype(jnp.float32)
        both = jnp.concatenate([high, v - high], axis=0)
        part = jnp.floor(cells * (1.0 / HALF))
        inner = cells - part * HALF
        left = jnp.concatenate(
            [jnp.where(part == float(h), both, 0.0).astype(jnp.bfloat16) for h in range(parts)],
            axis=0,
        )
        right = jnp.where(code == inner, 1.0, 0.0).astype(jnp.bfloat16)
        return left, right

    def bin_group(pairs):
        left = jnp.concatenate([a for a, _ in pairs], axis=1)
        right = jnp.concatenate([b for _, b in pairs], axis=1)
        acc[...] += lax.dot_general(
            left, right, (((1,), (1,)), ((), ())), preferred_element_type=jnp.float32
        )

    acc[...] = jnp.zeros_like(acc)

    def bin_own(g, carry):
        pairs = []
        for i in range(GROUP):
            b = g * GROUP + i
            cells = pool[b, pl.ds(field_count, 1), :] + offsets[pl.ds(b, 1), :]
            pairs.append(operands(pool[b], cells))
        bin_group(pairs)
        return carry

    lax.fori_loop(0, blocks // GROUP, bin_own, 0)

    def bin_got(got, first, count, base):
        pairs = []
        for i in range(first, first + count):
            cells = got[i, pl.ds(field_count, 1), :] + offsets[pl.ds(base + i, 1), :]
            pairs.append(operands(got[i], cells))
        bin_group(pairs)

    for copy in copies_x:
        copy.wait_recv()
    for slot in range(2 * CAP_X):
        pool[blocks + slot] = got_x[slot]
    for slot in range(2 * CAP_Z):
        fill(sent_z, slot, CAP_Z, 2 * CAP_X, 2)
    copies_z = exchange("gz", 2, sent_z, got_z, CAP_Z)
    bin_got(got_x, 0, 2 * CAP_X, blocks)

    for side in (0, 1):
        pltpu.make_async_remote_copy(
            src_ref=sent_z.at[pl.ds((1 - side) * CAP_Z, CAP_Z)],
            dst_ref=got_z.at[pl.ds(side * CAP_Z, CAP_Z)],
            send_sem=send_sem.at[3 - side],
            recv_sem=recv_sem.at[2 + side],
            device_id=upper["gz"] if side == 0 else lower["gz"],
            device_id_type=pl.DeviceIdType.MESH,
        ).wait_recv()
        bin_got(got_z, side * CAP_Z, CAP_Z, blocks + 2 * CAP_X)

    def total(kind):
        halves = []
        for h in range(kind * CELLS // HALF, (kind + 1) * CELLS // HALF):
            top = 2 * rows * h
            halves.append(acc[pl.ds(top, rows), :] + acc[pl.ds(top + rows, rows), :])
        return jnp.concatenate(halves, axis=1)

    sent_y[0] = total(1)
    sent_y[1] = total(2)
    copies_y = exchange("gy", 4, sent_y, got_y, 1)
    kept = total(0)
    for copy in copies_y:
        copy.wait_recv()
    out_ref[...] = (kept + got_y[0] + got_y[1])[:field_count]
    for copy in copies_x + copies_z + copies_y:
        copy.wait_send()


def solution(mesh):
    sizes = {axis: mesh.shape[axis] for axis in ("gx", "gy", "gz")}

    def per_device(particle_fields, step_length, live_mask, dest_cell, block_counts, block_lists):
        field_count, particles = particle_fields.shape
        blocks = particles // LANES
        rows = (field_count + 1 + 7) // 8 * 8
        pool_blocks = blocks + 2 * CAP_X + 2 * CAP_Z
        by_block = [a.reshape(blocks, LANES) for a in (step_length, live_mask, dest_cell)]
        any_space = pl.BlockSpec(memory_space=pl.ANY)
        vmem = pl.BlockSpec(memory_space=pltpu.VMEM)
        smem = pl.BlockSpec(memory_space=pltpu.SMEM)
        f32 = jnp.float32
        return pl.pallas_call(
            functools.partial(migrate_kernel, sizes),
            out_shape=jax.ShapeDtypeStruct((field_count, CELLS), f32),
            in_specs=[smem, smem, vmem, any_space, any_space, any_space, any_space],
            out_specs=vmem,
            scratch_shapes=[
                pltpu.VMEM((field_count, particles), f32),
                pltpu.VMEM((blocks, LANES), f32),
                pltpu.VMEM((blocks, LANES), jnp.int32),
                pltpu.VMEM((blocks, LANES), jnp.int32),
                pltpu.VMEM((blocks + 2 * CAP_X, rows, LANES), f32),
                pltpu.VMEM((pool_blocks, LANES), f32),
                pltpu.VMEM((2 * rows * CLASSES * CELLS // HALF, HALF), f32),
                pltpu.VMEM((2 * CAP_X, rows, LANES), f32),
                pltpu.VMEM((2 * CAP_Z, rows, LANES), f32),
                pltpu.VMEM((2 * CAP_X, rows, LANES), f32),
                pltpu.VMEM((2 * CAP_Z, rows, LANES), f32),
                pltpu.VMEM((2, rows, CELLS), f32),
                pltpu.VMEM((2, rows, CELLS), f32),
                pltpu.SemaphoreType.DMA((4,)),
                pltpu.SemaphoreType.DMA((6,)),
                pltpu.SemaphoreType.DMA((6,)),
            ],
            compiler_params=pltpu.CompilerParams(collective_id=0, has_side_effects=True),
        )(block_counts, block_lists, block_lists, particle_fields, *by_block)

    placed = (
        P(None, ("gx", "gy", "gz")),
        P(("gx", "gy", "gz")),
        P(("gx", "gy", "gz")),
        P(("gx", "gy", "gz")),
        P(("gx", "gy", "gz"), None),
        P(("gx", "gy", "gz"), None),
    )
    return jax.shard_map(
        per_device,
        mesh=mesh,
        in_specs=placed,
        out_specs=P(None, ("gx", "gy", "gz")),
        check_vma=False,
    )
```

```python
import functools

import jax
import jax.numpy as jnp
from jax import lax
from jax.experimental import pallas as pl
from jax.experimental.pallas import tpu as pltpu
from jax.sharding import PartitionSpec as P

CELLS = 512
CAP_X = 6
CAP_Z = 6
CAP_Y = 12
LANES = 128
HALF = 256
GROUP = 8
GONE = 8 * CELLS
CLASSES = 3


def migrate_kernel(
    sizes,
    counts,
    lists,
    lists_row,
    fields_hbm,
    step_hbm,
    live_hbm,
    cell_hbm,
    out_ref,
    fields,
    step,
    live,
    cell,
    pool,
    offsets,
    acc,
    sent_x,
    sent_z,
    got_x,
    got_z,
    sent_y,
    got_y,
    load_sem,
    send_sem,
    recv_sem,
):
    field_count = fields_hbm.shape[0]
    rows = pool.shape[1]
    whole = field_count // 8 * 8
    tail = field_count - whole
    blocks = step.shape[0]

    me = {axis: lax.axis_index(axis) for axis in ("gx", "gy", "gz")}
    lower = {axis: {axis: lax.rem(me[axis] + sizes[axis] - 1, sizes[axis])} for axis in me}
    upper = {axis: {axis: lax.rem(me[axis] + 1, sizes[axis])} for axis in me}

    loads = [
        pltpu.make_async_copy(fields_hbm, fields, load_sem.at[0]),
        pltpu.make_async_copy(step_hbm, step, load_sem.at[1]),
        pltpu.make_async_copy(live_hbm, live, load_sem.at[2]),
        pltpu.make_async_copy(cell_hbm, cell, load_sem.at[3]),
    ]
    for load in loads:
        load.start()

    barrier = pltpu.get_barrier_semaphore()
    for axis in me:
        for neighbour in (lower[axis], upper[axis]):
            pl.semaphore_signal(
                barrier, inc=1, device_id=neighbour, device_id_type=pl.DeviceIdType.MESH
            )

    spans = (CAP_X, CAP_X, CAP_Z, CAP_Z, CAP_Y, CAP_Y)
    lane = lax.broadcasted_iota(jnp.int32, lists_row.shape, 1)
    limit = jnp.zeros(lists_row.shape, jnp.int32)
    away = jnp.zeros(lists_row.shape, jnp.float32)
    start = 0
    for k, span in enumerate(spans):
        here = lane >= start
        limit = jnp.where(here, counts[0, k] + start, limit)
        away = jnp.where(here, float(GONE if k < 4 else (k - 3) * CELLS), away)
        start += span
    away = jnp.where(lane < limit, away, 0.0)
    number = lax.broadcasted_iota(jnp.int32, (offsets.shape[0], lists_row.shape[1]), 0)
    named = jnp.where(lists_row[...] == number, away, 0.0)
    offsets[...] = jnp.broadcast_to(jnp.sum(named, axis=1, keepdims=True), offsets.shape)

    for load in loads:
        load.wait()

    first_row = lax.broadcasted_iota(jnp.int32, (8, LANES), 0)

    def own_block(e):
        v = fields[:, pl.ds(pl.multiple_of(e * LANES, LANES), LANES)]
        top = v[:8]
        pace = step[pl.ds(e, 1), :]
        top = top + jnp.where(first_row < 3, pace * pltpu.roll(top, 5, 0), 0.0)
        v = jnp.concatenate([top, v[8:]], axis=0)
        v = v * live[pl.ds(e, 1), :].astype(jnp.float32)
        where_to = cell[pl.ds(e, 1), :].astype(jnp.float32)
        return jnp.concatenate(
            [v, jnp.broadcast_to(where_to, (rows - field_count, LANES))], axis=0
        )

    def exchange(axis, index, sent, got, width):
        out = []
        for side, (target, other) in enumerate(((lower, 1), (upper, 0))):
            copy = pltpu.make_async_remote_copy(
                src_ref=sent.at[pl.ds(side * width, width)],
                dst_ref=got.at[pl.ds(other * width, width)],
                send_sem=send_sem.at[index + side],
                recv_sem=recv_sem.at[index + other],
                device_id=target[axis],
                device_id_type=pl.DeviceIdType.MESH,
            )
            copy.start()
            out.append(copy)
        return out

    def fill(sent, slot, span, first_entry, first_count):
        count = jnp.full((rows, LANES), counts[0, first_count + slot // span])
        block = pool[lists[0, first_entry + slot]]
        block = jnp.where(count > slot % span, block, 0.0)
        side, i = slot // span, slot % span
        sent[side, pl.ds(i * whole, whole), :] = block[:whole]
        tail_at = span * whole + i * tail
        sent[side, pl.ds(tail_at, tail), :] = block[whole:field_count]
        sent[side, pl.ds(span * field_count + i, 1), :] = block[field_count : field_count + 1]

    def unpacked(got, slot, span):
        side, i = slot // span, slot % span
        body = got[side, pl.ds(i * whole, whole), :]
        rest = got[side, pl.ds(span * whole + i * tail, tail), :]
        cells = got[side, pl.ds(span * field_count + i, 1), :]
        spare = jnp.broadcast_to(cells, (rows - field_count, LANES))
        return jnp.concatenate([body, rest, spare], axis=0), cells

    def advance(g, carry):
        for i in range(GROUP):
            pool[g * GROUP + i] = own_block(g * GROUP + i)
        return carry

    lax.fori_loop(0, blocks // GROUP, advance, 0)
    for slot in range(2 * CAP_X):
        fill(sent_x, slot, CAP_X, 0, 0)
    pl.semaphore_wait(barrier, 6)
    copies_x = exchange("gx", 0, sent_x, got_x, 1)

    code = lax.broadcasted_iota(jnp.int32, (HALF, LANES), 0).astype(jnp.float32)
    parts = CLASSES * CELLS // HALF

    def operands(v, cells, wanted=tuple(range(parts))):
        high = v.astype(jnp.bfloat16).astype(jnp.float32)
        both = jnp.concatenate([high, v - high], axis=0)
        part = jnp.floor(cells * (1.0 / HALF))
        inner = cells - part * HALF
        left = jnp.concatenate(
            [jnp.where(part == float(h), both, 0.0).astype(jnp.bfloat16) for h in wanted],
            axis=0,
        )
        right = jnp.where(code == inner, 1.0, 0.0).astype(jnp.bfloat16)
        return left, right

    def bin_group(pairs):
        left = jnp.concatenate([a for a, _ in pairs], axis=1)
        right = jnp.concatenate([b for _, b in pairs], axis=1)
        acc[...] += lax.dot_general(
            left, right, (((1,), (1,)), ((), ())), preferred_element_type=jnp.float32
        )

    acc[...] = jnp.zeros_like(acc)

    def bin_own(g, carry):
        pairs = []
        for i in range(GROUP):
            b = g * GROUP + i
            cells = pool[b, pl.ds(field_count, 1), :] + offsets[pl.ds(b, 1), :]
            pairs.append(operands(pool[b], cells))
        bin_group(pairs)
        return carry

    early = 3 * (blocks // GROUP) // 8
    lax.fori_loop(0, early, bin_own, 0)

    def bin_got(got, side, width, base, wanted=tuple(range(parts))):
        pairs = []
        for i in range(side * width, (side + 1) * width):
            v, cells = unpacked(got, i, width)
            pairs.append(operands(v, cells + offsets[pl.ds(base + i, 1), :], wanted))
        left = jnp.concatenate([a for a, _ in pairs], axis=1)
        right = jnp.concatenate([b for _, b in pairs], axis=1)
        acc[pl.ds(2 * rows * wanted[0], 2 * rows * len(wanted)), :] += lax.dot_general(
            left, right, (((1,), (1,)), ((), ())), preferred_element_type=jnp.float32
        )

    for copy in copies_x:
        copy.wait_recv()
    for slot in range(2 * CAP_X):
        pool[blocks + slot] = unpacked(got_x, slot, CAP_X)[0]
    for slot in range(2 * CAP_Z):
        fill(sent_z, slot, CAP_Z, 2 * CAP_X, 2)
    copies_z = exchange("gz", 2, sent_z, got_z, 1)
    lax.fori_loop(early, blocks // GROUP, bin_own, 0)
    bin_got(got_x, 0, CAP_X, blocks)
    bin_got(got_x, 1, CAP_X, blocks)

    kept_parts = tuple(range(CELLS // HALF))
    bound_parts = tuple(range(CELLS // HALF, parts))
    late = blocks + 2 * CAP_X
    for side in (1, 0):
        pltpu.make_async_remote_copy(
            src_ref=sent_z.at[pl.ds(1 - side, 1)],
            dst_ref=got_z.at[pl.ds(side, 1)],
            send_sem=send_sem.at[3 - side],
            recv_sem=recv_sem.at[2 + side],
            device_id=upper["gz"] if side == 0 else lower["gz"],
            device_id_type=pl.DeviceIdType.MESH,
        ).wait_recv()
        if side == 1:
            bin_got(got_z, side, CAP_Z, late)
        else:
            bin_got(got_z, side, CAP_Z, late, bound_parts)

    def bin_kept(base):
        bin_got(got_z, 0, CAP_Z, base, kept_parts)

    def halves(kind):
        tops = [2 * rows * h for h in range(kind * CELLS // HALF, (kind + 1) * CELLS // HALF)]
        return [
            (acc[pl.ds(t, rows), :] + acc[pl.ds(t + rows, rows), :])[:field_count] for t in tops
        ]

    for side in (0, 1):
        for i, half in enumerate(halves(side + 1)):
            sent_y[side, pl.ds(i * field_count, field_count), :] = half
    copies_y = exchange("gy", 4, sent_y, got_y, 1)
    bin_kept(late)
    kept = halves(0)
    for copy in copies_y:
        copy.wait_recv()
    for i, half in enumerate(kept):
        part = pl.ds(i * field_count, field_count)
        out_ref[:, pl.ds(i * HALF, HALF)] = half + got_y[0, part, :] + got_y[1, part, :]
    for copy in copies_x + copies_z + copies_y:
        copy.wait_send()


def solution(mesh):
    sizes = {axis: mesh.shape[axis] for axis in ("gx", "gy", "gz")}

    def per_device(particle_fields, step_length, live_mask, dest_cell, block_counts, block_lists):
        field_count, particles = particle_fields.shape
        blocks = particles // LANES
        rows = (field_count + 1 + 7) // 8 * 8
        sum_rows = (field_count * CELLS // HALF + 7) // 8 * 8
        pool_blocks = blocks + 2 * CAP_X + 2 * CAP_Z

        def packed(span):
            return (span * (field_count + 1) + 7) // 8 * 8

        by_block = [a.reshape(blocks, LANES) for a in (step_length, live_mask, dest_cell)]
        any_space = pl.BlockSpec(memory_space=pl.ANY)
        vmem = pl.BlockSpec(memory_space=pltpu.VMEM)
        smem = pl.BlockSpec(memory_space=pltpu.SMEM)
        f32 = jnp.float32
        return pl.pallas_call(
            functools.partial(migrate_kernel, sizes),
            out_shape=jax.ShapeDtypeStruct((field_count, CELLS), f32),
            in_specs=[smem, smem, vmem, any_space, any_space, any_space, any_space],
            out_specs=vmem,
            scratch_shapes=[
                pltpu.VMEM((field_count, particles), f32),
                pltpu.VMEM((blocks, LANES), f32),
                pltpu.VMEM((blocks, LANES), jnp.int32),
                pltpu.VMEM((blocks, LANES), jnp.int32),
                pltpu.VMEM((blocks + 2 * CAP_X, rows, LANES), f32),
                pltpu.VMEM((pool_blocks, LANES), f32),
                pltpu.VMEM((2 * rows * CLASSES * CELLS // HALF, HALF), f32),
                pltpu.VMEM((2, packed(CAP_X), LANES), f32),
                pltpu.VMEM((2, packed(CAP_Z), LANES), f32),
                pltpu.VMEM((2, packed(CAP_X), LANES), f32),
                pltpu.VMEM((2, packed(CAP_Z), LANES), f32),
                pltpu.VMEM((2, sum_rows, HALF), f32),
                pltpu.VMEM((2, sum_rows, HALF), f32),
                pltpu.SemaphoreType.DMA((4,)),
                pltpu.SemaphoreType.DMA((6,)),
                pltpu.SemaphoreType.DMA((6,)),
            ],
            compiler_params=pltpu.CompilerParams(collective_id=0, has_side_effects=True),
        )(block_counts, block_lists, block_lists, particle_fields, *by_block)

    placed = (
        P(None, ("gx", "gy", "gz")),
        P(("gx", "gy", "gz")),
        P(("gx", "gy", "gz")),
        P(("gx", "gy", "gz")),
        P(("gx", "gy", "gz"), None),
        P(("gx", "gy", "gz"), None),
    )
    return jax.shard_map(
        per_device,
        mesh=mesh,
        in_specs=placed,
        out_specs=P(None, ("gx", "gy", "gz")),
        check_vma=False,
    )
```
